32 devices in a mesh: row: 8 (over y, x, core), col: 4 (over z).
Axes of the slice: x: 2, y: 2, z: 4, core: 2. Of those that a mesh axis runs over, the one named last changes fastest.
Arguments:
- tokens: bfloat16 [48, 8192], P('row', 'col'), may hold values from -6 to 6
- gate_weight: bfloat16 [8192, 20480], P('col', 'row'), may hold values from -0.0625 to 0.0625
- up_weight: bfloat16 [8192, 20480], P('col', 'row'), may hold values from -0.0625 to 0.0625
- down_weight: bfloat16 [20480, 8192], P('row', 'col'), may hold values from -0.0390625 to 0.0390625
- keep_mask: int32 [48, 20480], P('col', 'row'), may hold values 0 or 1
- cotangent: bfloat16 [48, 8192], P('row', 'col'), may hold values from -6 to 6
Outputs:
- mixed_out: bfloat16 [48, 8192], P('row', 'col')
- input_grad: bfloat16 [48, 8192], P('row', 'col')
- gate_grad: bfloat16 [8192, 20480], P('col', 'row')
- up_grad: bfloat16 [8192, 20480], P('col', 'row')
- down_grad: bfloat16 [20480, 8192], P('row', 'col')
The draws below stay inside these ranges and needn't reach their ends.
All inputs are finite; a program needn't handle non-finite values. No bound on the sum of `keep_mask` on one device may be relied on, other than what follows from the above.
Results may differ from the reference program's by a relative error of at most 0.0049.
Values may be sent and summed in bfloat16 or wider, within the bound.
A program may use at most 128 MiB of HBM per device.

```python
import jax
import jax.numpy as jnp

D = 8192
FF = 20480
TOKENS = 48


def with_ends(result, key, smallest, largest):
    shape = result.shape
    spot = [jax.random.randint(jax.random.fold_in(key, axis), (), 0, shape[axis]) for axis in range(len(shape))]
    result = result.at[tuple(spot)].set(smallest)
    longest = shape.index(max(shape))
    spot[longest] = (spot[longest] + 1) % shape[longest]
    return result.at[tuple(spot)].set(largest)


def block_scale(rng, extent, pieces, low, largest):
    gain = 1.0
    for axis_at, parts in pieces:
        draws = jax.random.uniform(jax.random.fold_in(jax.random.fold_in(rng, 6), axis_at), (parts,), jnp.float32, low / len(pieces), largest / len(pieces))
        gain = gain * jnp.repeat(jnp.exp(draws), extent[axis_at] // parts).reshape((-1,) + (1,) * (len(extent) - 1 - axis_at))
    return gain


def normal_values(stream_key, shape, deviation, most, cuts=(), kind=jnp.bfloat16):
    entries = deviation * jax.random.normal(stream_key, shape, jnp.float32)
    if cuts:
        entries = entries * block_scale(stream_key, shape, cuts, -0.22, 0.18)
    return jnp.clip(entries, -most, most).astype(kind)


def setup_inputs(seed: int = 0) -> dict:
    streams_of = jax.random.split(jax.random.key(seed), 7)
    return {
        "tokens": normal_values(streams_of[0], (TOKENS, D), 1.0, 6.0, ((0, 8), (1, 4))),
        "gate_weight": normal_values(streams_of[1], (D, FF), D ** -0.5, 0.0625, ((0, 4), (1, 8))),
        "up_weight": normal_values(streams_of[2], (D, FF), D ** -0.5, 0.0625, ((0, 4), (1, 8))),
        "down_weight": normal_values(streams_of[3], (FF, D), FF ** -0.5, 0.0390625, ((0, 8), (1, 4))),
        "keep_mask": with_ends((jax.random.randint(streams_of[4], (TOKENS, FF), 0, 10) < 9).astype(jnp.int32), jax.random.fold_in(streams_of[4], 1), 0, 1),
        "cotangent": normal_values(streams_of[5], (TOKENS, D), 1.0, 6.0, ((0, 8), (1, 4))),
    }


keep_scale = 1.0 / 0.9


def reference(tokens, gate_weight, up_weight, down_weight, keep_mask, cotangent):
    gate_value = jnp.dot(tokens, gate_weight, preferred_element_type=jnp.float32)
    up_value = jnp.dot(tokens, up_weight, preferred_element_type=jnp.float32)
    keep_factor = keep_mask.astype(jnp.float32) * keep_scale
    sigmoid_gate = jax.nn.sigmoid(gate_value)
    silu_gate = gate_value * sigmoid_gate
    hidden = (silu_gate * up_value * keep_factor).astype(jnp.bfloat16)
    mixed_out = jnp.dot(hidden, down_weight, preferred_element_type=jnp.float32).astype(jnp.bfloat16)
    grad_hidden = jnp.dot(cotangent, down_weight.T, preferred_element_type=jnp.float32)
    down_grad = jnp.dot(hidden.T, cotangent, preferred_element_type=jnp.float32).astype(jnp.bfloat16)
    grad_pre = grad_hidden * keep_factor
    grad_gate = (grad_pre * up_value * sigmoid_gate * (1.0 + gate_value * (1.0 - sigmoid_gate))).astype(jnp.bfloat16)
    grad_up = (grad_pre * silu_gate).astype(jnp.bfloat16)
    gate_grad = jnp.dot(tokens.T, grad_gate, preferred_element_type=jnp.float32).astype(jnp.bfloat16)
    up_grad = jnp.dot(tokens.T, grad_up, preferred_element_type=jnp.float32).astype(jnp.bfloat16)
    input_sum = jnp.dot(grad_gate, gate_weight.T, preferred_element_type=jnp.float32)
    input_sum = input_sum + jnp.dot(grad_up, up_weight.T, preferred_element_type=jnp.float32)
    input_grad = input_sum.astype(jnp.bfloat16)
    return mixed_out, input_grad, gate_grad, up_grad, down_grad
```

```python
import functools

import jax
import jax.numpy as jnp
from jax import lax
from jax.experimental import pallas as pl
from jax.experimental.pallas import tpu as pltpu
from jax.sharding import PartitionSpec as P

keep_scale = 1.0 / 0.9
contract_last = (((1,), (1,)), ((), ()))
contract_first = (((0,), (0,)), ((), ()))
f32 = jnp.float32
bf16 = jnp.bfloat16
MESH = pl.DeviceIdType.MESH


def project_in(tokens, gate_weight, up_weight):
    gathered = lax.all_gather(tokens, "row", axis=0, tiled=True)
    gate_part = jnp.dot(gathered, gate_weight, preferred_element_type=f32)
    up_part = jnp.dot(gathered, up_weight, preferred_element_type=f32)
    gate_value, up_value = lax.psum((gate_part, up_part), "col")
    return (gathered, gate_value, up_value)


def plain_body(tokens, gate_weight, up_weight, down_weight, keep_mask, cotangent):
    gathered, gate_value, up_value = project_in(tokens, gate_weight, up_weight)
    mask_all = lax.all_gather(keep_mask, "col", axis=0, tiled=True)
    keep_factor = mask_all.astype(f32) * keep_scale
    sigmoid_gate = jax.nn.sigmoid(gate_value)
    silu_gate = gate_value * sigmoid_gate
    hidden = (silu_gate * up_value * keep_factor).astype(bf16)
    mixed_out = lax.psum_scatter(
        jnp.dot(hidden, down_weight, preferred_element_type=f32),
        "row",
        scatter_dimension=0,
        tiled=True,
    ).astype(bf16)
    cot_all = lax.all_gather(cotangent, "row", axis=0, tiled=True)
    hidden_part = lax.dot_general(cot_all, down_weight, contract_last, preferred_element_type=f32)
    grad_hidden = lax.psum(hidden_part, "col")
    down_grad = lax.dot_general(
        hidden, cot_all, contract_first, preferred_element_type=f32
    ).astype(bf16)
    grad_pre = grad_hidden * keep_factor
    grad_gate = (
        grad_pre * up_value * sigmoid_gate * (1.0 + gate_value * (1.0 - sigmoid_gate))
    ).astype(bf16)
    grad_up = (grad_pre * silu_gate).astype(bf16)
    gate_grad = lax.dot_general(
        gathered, grad_gate, contract_first, preferred_element_type=f32
    ).astype(bf16)
    up_grad = lax.dot_general(
        gathered, grad_up, contract_first, preferred_element_type=f32
    ).astype(bf16)
    first = lax.dot_general(grad_gate, gate_weight, contract_last, preferred_element_type=f32)
    second = lax.dot_general(grad_up, up_weight, contract_last, preferred_element_type=f32)
    input_grad = lax.psum_scatter(first + second, "row", scatter_dimension=0, tiled=True).astype(
        bf16
    )
    return (mixed_out, input_grad, gate_grad, up_grad, down_grad)


def one_hot(rows, cols, want):
    i = lax.broadcasted_iota(jnp.int32, (rows, cols), 0)
    j = lax.broadcasted_iota(jnp.int32, (rows, cols), 1)
    return jnp.where(want(i, j), 1.0, 0.0).astype(bf16)


def layer_kernel(R, C, tok_ref, cot_ref, mask_ref, gate_hbm, up_hbm, down_hbm,
                 mixed_ref, input_ref, tok_all, cot_all, act,
                 wgate, wup, wdown, wsem, pack, packed, gathered, x_send, x_recv,
                 mpad, mpacked, mall, m_send, m_recv,
                 part32, own, gh_out, gh_in, gu_in, p_send, p_recv,
                 a_send, a_recv, acc, rs_out, rs_in, r_send, r_recv):
    me_r = lax.axis_index("row")
    me_c = lax.axis_index("col")
    t, D = tok_ref.shape
    F = gate_hbm.shape[1]
    S = F // C
    T = R * t
    tm = mask_ref.shape[0]

    def peer_c(j):
        return lax.rem(me_c + 1 + j, C)

    def cols(p):
        return pl.ds(pl.multiple_of(p * S, 128), S)

    def weight_copy(a, j):
        p = peer_c(j)
        src, dst = ((down_hbm.at[cols(p), :], wdown), (gate_hbm.at[:, cols(p)], wgate),
                    (up_hbm.at[:, cols(p)], wup))[a]
        return pltpu.make_async_copy(src, dst.at[j], wsem.at[a, j])

    for a in range(3):
        for j in range(C):
            weight_copy(a, j).start()

    barrier = pltpu.get_barrier_semaphore()
    for k in range(1, R):
        pl.semaphore_signal(barrier, inc=1, device_id={"row": lax.rem(me_r + k, R)}, device_id_type=MESH)
    for k in range(1, C):
        pl.semaphore_signal(barrier, inc=1, device_id={"col": lax.rem(me_c + k, C)}, device_id_type=MESH)

    pack[...] = jnp.zeros_like(pack)
    pack[0:t, :] = tok_ref[...].astype(f32)
    pack[8:8 + t, :] = cot_ref[...].astype(f32)
    mine = pack[...].astype(bf16)
    packed[...] = mine
    gathered[me_r] = mine
    mpad[...] = jnp.zeros_like(mpad)
    mpad[0:tm, :] = mask_ref[...].astype(f32)
    mpacked[...] = mpad[...].astype(bf16)
    mall[me_c] = mpacked[:, cols(me_c)]

    pl.semaphore_wait(barrier, R - 1 + C - 1)

    def x_copy(k):
        return pltpu.make_async_remote_copy(
            src_ref=packed, dst_ref=gathered.at[me_r], send_sem=x_send.at[k], recv_sem=x_recv.at[k],
            device_id={"row": lax.rem(me_r + k, R)}, device_id_type=MESH)

    def m_copy(k):
        p = lax.rem(me_c + k, C)
        return pltpu.make_async_remote_copy(
            src_ref=mpacked.at[:, cols(p)], dst_ref=mall.at[me_c], send_sem=m_send.at[k],
            recv_sem=m_recv.at[k], device_id={"col": p}, device_id_type=MESH)

    for k in range(1, R):
        x_copy(k).start()
    for k in range(1, C):
        m_copy(k).start()
    for k in range(1, R):
        x_copy(k).wait_recv()

    flat = gathered[...].reshape(R * 16, D)
    pick = one_hot(T, R * 16, lambda i, j: j == (i // t) * 16 + i % t)
    tok_all[...] = jnp.dot(pick, flat, preferred_element_type=f32).astype(bf16)
    pick = one_hot(T, R * 16, lambda i, j: j == (i // t) * 16 + 8 + i % t)
    cot_all[...] = jnp.dot(pick, flat, preferred_element_type=f32).astype(bf16)

    def part_copy(a, j):
        src, dst = ((gh_out.at[j], gh_in.at[me_c]), (part32.at[0, j], gu_in.at[0, me_c]),
                    (part32.at[1, j], gu_in.at[1, me_c]))[a]
        return pltpu.make_async_remote_copy(
            src_ref=src, dst_ref=dst, send_sem=p_send.at[a, j], recv_sem=p_recv.at[a, j],
            device_id={"col": peer_c(j)}, device_id_type=MESH)

    def partial(a, j):
        weight_copy(a, j).wait()
        if a == 0:
            return lax.dot_general(cot_all[...], wdown[j], contract_last, preferred_element_type=f32)
        w = wgate if a == 1 else wup
        return jnp.dot(tok_all[...], w[j], preferred_element_type=f32)

    for a in range(3):
        def step(j, carry, a=a):
            value = partial(a, j)
            own[a] = value

            @pl.when(j < C - 1)
            def _():
                if a == 0:
                    gh_out[j] = value.astype(bf16)
                else:
                    part32[a - 1, j] = value
                part_copy(a, j).start()
            return carry
        lax.fori_loop(0, C, step, 0)

    for k in range(1, C):
        m_copy(k).wait_recv()
    pick = one_hot(T, C * 16, lambda i, j: j == (i // tm) * 16 + i % tm)
    keep = jnp.dot(pick, mall[...].reshape(C * 16, S), preferred_element_type=f32) * keep_scale
    gh = own[0]
    for j in range(C - 1):
        part_copy(0, j).wait_recv()
    for k in range(1, C):
        gh = gh + gh_in[lax.rem(me_c + k, C)].astype(f32)
    gate = own[1]
    for j in range(C - 1):
        part_copy(1, j).wait_recv()
    for k in range(1, C):
        gate = gate + gu_in[0, lax.rem(me_c + k, C)]
    up = own[2]
    for j in range(C - 1):
        part_copy(2, j).wait_recv()
    for k in range(1, C):
        up = up + gu_in[1, lax.rem(me_c + k, C)]
    sig = 1.0 / (1.0 + jnp.exp(-gate))
    silu = gate * sig
    pre = gh * keep
    act[me_c, 0] = (silu * up * keep).astype(bf16)
    act[me_c, 1] = (pre * up * sig * (1.0 + gate * (1.0 - sig))).astype(bf16)
    act[me_c, 2] = (pre * silu).astype(bf16)

    def act_copy(k):
        return pltpu.make_async_remote_copy(
            src_ref=act.at[me_c], dst_ref=act.at[me_c], send_sem=a_send.at[k], recv_sem=a_recv.at[k],
            device_id={"col": lax.rem(me_c + k, C)}, device_id_type=MESH)

    for k in range(1, C):
        act_copy(k).start()

    spread = one_hot(R * 8, T, lambda i, j: (j == (i // 8) * t + i % 8) & (i % 8 < t))
    acc[...] = jnp.zeros_like(acc)

    def widen(value):
        return jnp.dot(spread, value, preferred_element_type=f32).astype(bf16)

    def back(k, carry):
        p = lax.rem(me_c + C - k, C)
        j = C - 1 - k

        @pl.when(k > 0)
        def _():
            act_copy(k).wait_recv()
        acc[0] += jnp.dot(widen(act[p, 0]), wdown[j], preferred_element_type=f32)
        acc[1] += lax.dot_general(
            widen(act[p, 1]), wgate[j], contract_last, preferred_element_type=f32
        ) + lax.dot_general(widen(act[p, 2]), wup[j], contract_last, preferred_element_type=f32)
        return carry
    lax.fori_loop(0, C, back, 0)

    def r_copy(k):
        p = lax.rem(me_r + k, R)
        return pltpu.make_async_remote_copy(
            src_ref=rs_out.at[k], dst_ref=rs_in.at[me_r], send_sem=r_send.at[k], recv_sem=r_recv.at[k],
            device_id={"row": p}, device_id_type=MESH)

    def rows(p):
        return pl.ds(pl.multiple_of(p * 8, 8), 8)

    for k in range(1, R):
        p = lax.rem(me_r + k, R)
        rs_out[k] = jnp.concatenate([acc[0, rows(p), :], acc[1, rows(p), :]], axis=0).astype(bf16)
        r_copy(k).start()
    total = jnp.concatenate([acc[0, rows(me_r), :], acc[1, rows(me_r), :]], axis=0)
    for k in range(1, R):
        r_copy(k).wait_recv()
    for k in range(1, R):
        total = total + rs_in[lax.rem(me_r + k, R)].astype(f32)
    mixed_ref[...] = total[0:t].astype(bf16)
    input_ref[...] = total[8:8 + t].astype(bf16)

    for k in range(1, R):
        x_copy(k).wait_send()
        r_copy(k).wait_send()
    for k in range(1, C):
        m_copy(k).wait_send()
        act_copy(k).wait_send()
    for a in range(3):
        for j in range(C - 1):
            part_copy(a, j).wait_send()


def outer_kernel(tok_ref, cot_ref, act_ref, gate_out, up_out, down_out):
    tok = tok_ref[...]
    gate_out[...] = lax.dot_general(
        tok, act_ref[0, 1], contract_first, preferred_element_type=f32).astype(bf16)
    up_out[...] = lax.dot_general(
        tok, act_ref[0, 2], contract_first, preferred_element_type=f32).astype(bf16)
    down_out[...] = lax.dot_general(
        act_ref[0, 0], cot_ref[...], contract_first, preferred_element_type=f32).astype(bf16)


def kernel_body(R, C, tokens, gate_weight, up_weight, down_weight, keep_mask, cotangent):
    t, D = tokens.shape
    F = gate_weight.shape[1]
    S = F // C
    T = R * t
    vm = pl.BlockSpec(memory_space=pltpu.VMEM)
    anyspec = pl.BlockSpec(memory_space=pl.ANY)
    dma = pltpu.SemaphoreType.DMA
    sds = jax.ShapeDtypeStruct
    V = pltpu.VMEM
    mixed, input_grad, tok_all, cot_all, act = pl.pallas_call(
        functools.partial(layer_kernel, R, C),
        name="layer",
        out_shape=(sds((t, D), bf16), sds((t, D), bf16), sds((T, D), bf16), sds((T, D), bf16),
                   sds((C, 3, T, S), bf16)),
        in_specs=[vm, vm, vm, anyspec, anyspec, anyspec],
        out_specs=(vm,) * 5,
        scratch_shapes=[
            V((C, D, S), bf16), V((C, D, S), bf16), V((C, S, D), bf16), dma((3, C)),
            V((16, D), f32), V((16, D), bf16), V((R, 16, D), bf16), dma((R,)), dma((R,)),
            V((16, F), f32), V((16, F), bf16), V((C, 16, S), bf16), dma((C,)), dma((C,)),
            V((2, C, T, S), f32), V((3, T, S), f32), V((C, T, S), bf16), V((C, T, S), bf16),
            V((2, C, T, S), f32), dma((3, C)), dma((3, C)),
            dma((C,)), dma((C,)), V((2, R * 8, D), f32), V((R, 16, D), bf16), V((R, 16, D), bf16),
            dma((R,)), dma((R,)),
        ],
        compiler_params=pltpu.CompilerParams(
            collective_id=0, has_side_effects=True, vmem_limit_bytes=60 * 1024 * 1024),
    )(tokens, cotangent, keep_mask, gate_weight, up_weight, down_weight)
    split = 2 if D % 256 == 0 else 1
    H = D // split
    gate_grad, up_grad, down_grad = pl.pallas_call(
        outer_kernel,
        name="outer",
        grid=(C, split),
        out_shape=(sds((D, F), bf16), sds((D, F), bf16), sds((F, D), bf16)),
        in_specs=[
            pl.BlockSpec((T, H), lambda p, h: (0, h)),
            pl.BlockSpec((T, H), lambda p, h: (0, h)),
            pl.BlockSpec((1, 3, T, S), lambda p, h: (p, 0, 0, 0)),
        ],
        out_specs=(
            pl.BlockSpec((H, S), lambda p, h: (h, p)),
            pl.BlockSpec((H, S), lambda p, h: (h, p)),
            pl.BlockSpec((S, H), lambda p, h: (p, h)),
        ),
        compiler_params=pltpu.CompilerParams(vmem_limit_bytes=40 * 1024 * 1024),
    )(tok_all, cot_all, act)
    return mixed, input_grad, gate_grad, up_grad, down_grad


def body(R, C, tokens, gate_weight, up_weight, down_weight, keep_mask, cotangent):
    t, D = tokens.shape
    F = gate_weight.shape[1]
    tm = keep_mask.shape[0]
    fits = t <= 8 and tm <= 16 and F % (C * 128) == 0 and D % 128 == 0
    if fits:
        return kernel_body(R, C, tokens, gate_weight, up_weight, down_weight, keep_mask, cotangent)
    return plain_body(tokens, gate_weight, up_weight, down_weight, keep_mask, cotangent)


def solution(mesh):
    placed = (
        P("row", "col"),
        P("col", "row"),
        P("col", "row"),
        P("row", "col"),
        P("col", "row"),
        P("row", "col"),
    )
    return jax.shard_map(
        functools.partial(body, mesh.shape["row"], mesh.shape["col"]),
        mesh=mesh,
        in_specs=placed,
        out_specs=(
            P("row", "col"),
            P("row", "col"),
            P("col", "row"),
            P("col", "row"),
            P("row", "col"),
        ),
        check_vma=False,
    )
```

```python
import functools

import jax
import jax.numpy as jnp
from jax import lax
from jax.experimental import pallas as pl
from jax.experimental.pallas import tpu as pltpu
from jax.sharding import PartitionSpec as P

keep_scale = 1.0 / 0.9
contract_last = (((1,), (1,)), ((), ()))
contract_first = (((0,), (0,)), ((), ()))
f32 = jnp.float32
bf16 = jnp.bfloat16
MESH = pl.DeviceIdType.MESH


def project_in(tokens, gate_weight, up_weight):
    gathered = lax.all_gather(tokens, "row", axis=0, tiled=True)
    gate_part = jnp.dot(gathered, gate_weight, preferred_element_type=f32)
    up_part = jnp.dot(gathered, up_weight, preferred_element_type=f32)
    gate_value, up_value = lax.psum((gate_part, up_part), "col")
    return (gathered, gate_value, up_value)


def plain_body(tokens, gate_weight, up_weight, down_weight, keep_mask, cotangent):
    gathered, gate_value, up_value = project_in(tokens, gate_weight, up_weight)
    mask_all = lax.all_gather(keep_mask, "col", axis=0, tiled=True)
    keep_factor = mask_all.astype(f32) * keep_scale
    sigmoid_gate = jax.nn.sigmoid(gate_value)
    silu_gate = gate_value * sigmoid_gate
    hidden = (silu_gate * up_value * keep_factor).astype(bf16)
    mixed_out = lax.psum_scatter(
        jnp.dot(hidden, down_weight, preferred_element_type=f32),
        "row",
        scatter_dimension=0,
        tiled=True,
    ).astype(bf16)
    cot_all = lax.all_gather(cotangent, "row", axis=0, tiled=True)
    hidden_part = lax.dot_general(cot_all, down_weight, contract_last, preferred_element_type=f32)
    grad_hidden = lax.psum(hidden_part, "col")
    down_grad = lax.dot_general(
        hidden, cot_all, contract_first, preferred_element_type=f32
    ).astype(bf16)
    grad_pre = grad_hidden * keep_factor
    grad_gate = (
        grad_pre * up_value * sigmoid_gate * (1.0 + gate_value * (1.0 - sigmoid_gate))
    ).astype(bf16)
    grad_up = (grad_pre * silu_gate).astype(bf16)
    gate_grad = lax.dot_general(
        gathered, grad_gate, contract_first, preferred_element_type=f32
    ).astype(bf16)
    up_grad = lax.dot_general(
        gathered, grad_up, contract_first, preferred_element_type=f32
    ).astype(bf16)
    first = lax.dot_general(grad_gate, gate_weight, contract_last, preferred_element_type=f32)
    second = lax.dot_general(grad_up, up_weight, contract_last, preferred_element_type=f32)
    input_grad = lax.psum_scatter(first + second, "row", scatter_dimension=0, tiled=True).astype(
        bf16
    )
    return (mixed_out, input_grad, gate_grad, up_grad, down_grad)


def one_hot(rows, cols, want):
    i = lax.broadcasted_iota(jnp.int32, (rows, cols), 0)
    j = lax.broadcasted_iota(jnp.int32, (rows, cols), 1)
    return jnp.where(want(i, j), 1.0, 0.0).astype(bf16)


def layer_kernel(R, C, tok_ref, cot_ref, mask_ref, gate_hbm, up_hbm, down_hbm,
                 mixed_ref, input_ref, tok_all, cot_all, act,
                 wgate, wup, wdown, wsem, pack, packed, gathered, x_send, x_recv,
                 mpad, mpacked, mall, m_send, m_recv,
                 part32, own, part16, pair_in, gate_in, p_send, p_recv,
                 a_send, a_recv, acc, rs_out, rs_in, r_send, r_recv):
    me_r = lax.axis_index("row")
    me_c = lax.axis_index("col")
    t, D = tok_ref.shape
    F = gate_hbm.shape[1]
    S = F // C
    T = R * t
    tm = mask_ref.shape[0]

    def peer_c(j):
        return lax.rem(me_c + 1 + j, C)

    def cols(p):
        return pl.ds(pl.multiple_of(p * S, 128), S)

    def weight_copy(a, j):
        p = peer_c(j)
        src, dst = ((gate_hbm.at[:, cols(p)], wgate), (up_hbm.at[:, cols(p)], wup),
                    (down_hbm.at[cols(p), :], wdown))[a]
        return pltpu.make_async_copy(src, dst.at[j], wsem.at[a, j])

    for a in range(3):
        for j in range(C):
            weight_copy(a, j).start()

    barrier = pltpu.get_barrier_semaphore()
    for k in range(1, R):
        pl.semaphore_signal(barrier, inc=1, device_id={"row": lax.rem(me_r + k, R)}, device_id_type=MESH)
    for k in range(1, C):
        pl.semaphore_signal(barrier, inc=1, device_id={"col": lax.rem(me_c + k, C)}, device_id_type=MESH)

    pack[...] = jnp.zeros_like(pack)
    pack[0:t, :] = tok_ref[...].astype(f32)
    pack[8:8 + t, :] = cot_ref[...].astype(f32)
    mine = pack[...].astype(bf16)
    packed[...] = mine
    gathered[me_r] = mine
    mpad[...] = jnp.zeros_like(mpad)
    mpad[0:tm, :] = mask_ref[...].astype(f32)
    mpacked[...] = mpad[...].astype(bf16)
    mall[me_c] = mpacked[:, cols(me_c)]

    pl.semaphore_wait(barrier, R - 1 + C - 1)

    def x_copy(k):
        return pltpu.make_async_remote_copy(
            src_ref=packed, dst_ref=gathered.at[me_r], send_sem=x_send.at[k], recv_sem=x_recv.at[k],
            device_id={"row": lax.rem(me_r + k, R)}, device_id_type=MESH)

    def m_copy(k):
        p = lax.rem(me_c + k, C)
        return pltpu.make_async_remote_copy(
            src_ref=mpacked.at[:, cols(p)], dst_ref=mall.at[me_c], send_sem=m_send.at[k],
            recv_sem=m_recv.at[k], device_id={"col": p}, device_id_type=MESH)

    for k in range(1, R):
        x_copy(k).start()
    for k in range(1, C):
        m_copy(k).start()
    for k in range(1, R):
        x_copy(k).wait_recv()

    flat = gathered[...].reshape(R * 16, D)
    pick = one_hot(T, R * 16, lambda i, j: j == (i // t) * 16 + i % t)
    tok_all[...] = jnp.dot(pick, flat, preferred_element_type=f32).astype(bf16)
    pick = one_hot(T, R * 16, lambda i, j: j == (i // t) * 16 + 8 + i % t)
    cot_all[...] = jnp.dot(pick, flat, preferred_element_type=f32).astype(bf16)

    def part_copy(a, j):
        if a == 0:
            src, dst = part32.at[j], gate_in.at[me_c]
        else:
            src, dst = part16.at[a - 1, j], pair_in.at[a - 1, me_c]
        return pltpu.make_async_remote_copy(
            src_ref=src, dst_ref=dst, send_sem=p_send.at[a, j], recv_sem=p_recv.at[a, j],
            device_id={"col": peer_c(j)}, device_id_type=MESH)

    def partial(a, j):
        weight_copy(a, j).wait()
        if a == 2:
            return lax.dot_general(cot_all[...], wdown[j], contract_last, preferred_element_type=f32)
        w = wgate if a == 0 else wup
        return jnp.dot(tok_all[...], w[j], preferred_element_type=f32)

    for a in range(3):
        def step(j, carry, a=a):
            value = partial(a, j)
            own[a] = value

            @pl.when(j < C - 1)
            def _():
                if a == 0:
                    part32[j] = value
                else:
                    part16[a - 1, j] = value.astype(bf16)
                part_copy(a, j).start()
            return carry
        lax.fori_loop(0, C, step, 0)

    for k in range(1, C):
        m_copy(k).wait_recv()
    pick = one_hot(T, C * 16, lambda i, j: j == (i // tm) * 16 + i % tm)
    keep = jnp.dot(pick, mall[...].reshape(C * 16, S), preferred_element_type=f32) * keep_scale
    def act_copy(n, k):
        return pltpu.make_async_remote_copy(
            src_ref=act.at[me_c, n], dst_ref=act.at[me_c, n], send_sem=a_send.at[n, k],
            recv_sem=a_recv.at[n, k], device_id={"col": lax.rem(me_c + k, C)}, device_id_type=MESH)

    def summed(a):
        value = own[a]
        for j in range(C - 1):
            part_copy(a, j).wait_recv()
        for k in range(1, C):
            p = lax.rem(me_c + k, C)
            value = value + (gate_in[p] if a == 0 else pair_in[a - 1, p].astype(f32))
        return value

    gate = summed(0)
    up = summed(1)
    sig = 1.0 / (1.0 + jnp.exp(-gate))
    silu = gate * sig
    act[me_c, 0] = (silu * up * keep).astype(bf16)
    for k in range(1, C):
        act_copy(0, k).start()
    pre = summed(2) * keep
    act[me_c, 1] = (pre * up * sig * (1.0 + gate * (1.0 - sig))).astype(bf16)
    act[me_c, 2] = (pre * silu).astype(bf16)
    for n in (1, 2):
        for k in range(1, C):
            act_copy(n, k).start()

    spread = one_hot(R * 8, T, lambda i, j: (j == (i // 8) * t + i % 8) & (i % 8 < t))
    acc[...] = jnp.zeros_like(acc)

    def widen(value):
        return jnp.dot(spread, value, preferred_element_type=f32).astype(bf16)

    def back_mixed(k, carry):
        p = lax.rem(me_c + C - k, C)

        @pl.when(k > 0)
        def _():
            act_copy(0, k).wait_recv()
        acc[0] += jnp.dot(widen(act[p, 0]), wdown[C - 1 - k], preferred_element_type=f32)
        return carry

    def back_input(k, carry):
        p = lax.rem(me_c + C - k, C)
        j = C - 1 - k

        @pl.when(k > 0)
        def _():
            act_copy(1, k).wait_recv()
        acc[1] += lax.dot_general(
            widen(act[p, 1]), wgate[j], contract_last, preferred_element_type=f32)

        @pl.when(k > 0)
        def _():
            act_copy(2, k).wait_recv()
        acc[1] += lax.dot_general(
            widen(act[p, 2]), wup[j], contract_last, preferred_element_type=f32)
        return carry

    def r_copy(n, k):
        return pltpu.make_async_remote_copy(
            src_ref=rs_out.at[n, k], dst_ref=rs_in.at[n, me_r], send_sem=r_send.at[n, k],
            recv_sem=r_recv.at[n, k], device_id={"row": lax.rem(me_r + k, R)}, device_id_type=MESH)

    def rows(p):
        return pl.ds(pl.multiple_of(p * 8, 8), 8)

    def send_rows(n):
        for k in range(1, R):
            rs_out[n, k] = acc[n, rows(lax.rem(me_r + k, R)), :].astype(bf16)
            r_copy(n, k).start()

    def sum_rows(n):
        total = acc[n, rows(me_r), :]
        for k in range(1, R):
            r_copy(n, k).wait_recv()
        for k in range(1, R):
            total = total + rs_in[n, lax.rem(me_r + k, R)].astype(f32)
        return total[0:t].astype(bf16)

    lax.fori_loop(0, C, back_mixed, 0)
    send_rows(0)
    lax.fori_loop(0, C, back_input, 0)
    send_rows(1)
    mixed_ref[...] = sum_rows(0)
    input_ref[...] = sum_rows(1)

    for k in range(1, R):
        x_copy(k).wait_send()
        r_copy(0, k).wait_send()
        r_copy(1, k).wait_send()
    for k in range(1, C):
        m_copy(k).wait_send()
        for n in range(3):
            act_copy(n, k).wait_send()
    for a in range(3):
        for j in range(C - 1):
            part_copy(a, j).wait_send()


def outer_kernel(tok_ref, cot_ref, act_ref, mixed_ref, input_ref,
                 gate_out, up_out, down_out, mixed_out, input_out):
    mixed_out[...] = mixed_ref[...]
    input_out[...] = input_ref[...]
    tok = tok_ref[...]
    gate_out[...] = lax.dot_general(
        tok, act_ref[0, 1], contract_first, preferred_element_type=f32).astype(bf16)
    up_out[...] = lax.dot_general(
        tok, act_ref[0, 2], contract_first, preferred_element_type=f32).astype(bf16)
    down_out[...] = lax.dot_general(
        act_ref[0, 0], cot_ref[...], contract_first, preferred_element_type=f32).astype(bf16)


def kernel_body(R, C, tokens, gate_weight, up_weight, down_weight, keep_mask, cotangent):
    t, D = tokens.shape
    F = gate_weight.shape[1]
    S = F // C
    T = R * t
    vm = pl.BlockSpec(memory_space=pltpu.VMEM)
    anyspec = pl.BlockSpec(memory_space=pl.ANY)
    dma = pltpu.SemaphoreType.DMA
    sds = jax.ShapeDtypeStruct
    V = pltpu.VMEM
    mixed, input_grad, tok_all, cot_all, act = pl.pallas_call(
        functools.partial(layer_kernel, R, C),
        name="layer",
        out_shape=(sds((t, D), bf16), sds((t, D), bf16), sds((T, D), bf16), sds((T, D), bf16),
                   sds((C, 3, T, S), bf16)),
        in_specs=[vm, vm, vm, anyspec, anyspec, anyspec],
        out_specs=(vm,) * 5,
        scratch_shapes=[
            V((C, D, S), bf16), V((C, D, S), bf16), V((C, S, D), bf16), dma((3, C)),
            V((16, D), f32), V((16, D), bf16), V((R, 16, D), bf16), dma((R,)), dma((R,)),
            V((16, F), f32), V((16, F), bf16), V((C, 16, S), bf16), dma((C,)), dma((C,)),
            V((C, T, S), f32), V((3, T, S), f32), V((2, C, T, S), bf16), V((2, C, T, S), bf16),
            V((C, T, S), f32), dma((3, C)), dma((3, C)),
            dma((3, C)), dma((3, C)), V((2, R * 8, D), f32), V((2, R, 8, D), bf16),
            V((2, R, 8, D), bf16), dma((2, R)), dma((2, R)),
        ],
        compiler_params=pltpu.CompilerParams(
            collective_id=0, has_side_effects=True, vmem_limit_bytes=60 * 1024 * 1024),
    )(tokens, cotangent, keep_mask, gate_weight, up_weight, down_weight)
    split = 2 if D % 256 == 0 else 1
    H = D // split
    whole = pl.BlockSpec((t, D), lambda p, h: (0, 0))
    gate_grad, up_grad, down_grad, mixed, input_grad = pl.pallas_call(
        outer_kernel,
        name="outer",
        grid=(C, split),
        out_shape=(sds((D, F), bf16), sds((D, F), bf16), sds((F, D), bf16),
                   sds((t, D), bf16), sds((t, D), bf16)),
        in_specs=[
            pl.BlockSpec((T, H), lambda p, h: (0, h)),
            pl.BlockSpec((T, H), lambda p, h: (0, h)),
            pl.BlockSpec((1, 3, T, S), lambda p, h: (p, 0, 0, 0)),
            whole, whole,
        ],
        out_specs=(
            pl.BlockSpec((H, S), lambda p, h: (h, p)),
            pl.BlockSpec((H, S), lambda p, h: (h, p)),
            pl.BlockSpec((S, H), lambda p, h: (p, h)),
            whole, whole,
        ),
        compiler_params=pltpu.CompilerParams(vmem_limit_bytes=63 * 1024 * 1024),
    )(tok_all, cot_all, act, mixed, input_grad)
    return mixed, input_grad, gate_grad, up_grad, down_grad


def body(R, C, tokens, gate_weight, up_weight, down_weight, keep_mask, cotangent):
    t, D = tokens.shape
    F = gate_weight.shape[1]
    tm = keep_mask.shape[0]
    fits = t <= 8 and tm <= 16 and F % (C * 128) == 0 and D % 128 == 0
    if fits:
        return kernel_body(R, C, tokens, gate_weight, up_weight, down_weight, keep_mask, cotangent)
    return plain_body(tokens, gate_weight, up_weight, down_weight, keep_mask, cotangent)


def solution(mesh):
    placed = (
        P("row", "col"),
        P("col", "row"),
        P("col", "row"),
        P("row", "col"),
        P("col", "row"),
        P("row", "col"),
    )
    return jax.shard_map(
        functools.partial(body, mesh.shape["row"], mesh.shape["col"]),
        mesh=mesh,
        in_specs=placed,
        out_specs=(
            P("row", "col"),
            P("row", "col"),
            P("col", "row"),
            P("col", "row"),
            P("row", "col"),
        ),
        check_vma=False,
    )
```
